32 devices in a mesh: obs: 8 (over z, x), bel: 4 (over y, core).
Axes of the slice: x: 2, y: 2, z: 4, core: 2. Of those that a mesh axis runs over, the one named last changes fastest.
Arguments:
- alpha_set: bfloat16 [2048, 2048], P('bel'), may hold values from -600 to 600
- transitions: bfloat16 [16, 2048, 2048], P(None, 'obs'), may hold values from 0.0009994507 to 1
- obs_weights: float32 [256, 16, 2048], P('obs'), may hold values from 0.01 to 1
- rewards: float32 [16, 2048], replicated, may hold values from -1 to 1
- chosen_idx: int32 [1536, 16, 256], P('bel', None, 'obs'), may hold values from 0 to 2047
- chosen_action: int32 [1536], P('bel'), may hold values from 0 to 15
Outputs:
- new_alpha: float32 [1536, 2048], P(('bel', 'obs'))
The draws below stay inside these ranges and needn't reach their ends.
Inputs may be any that keep to these rules, and one draw needn't show every extreme that they name: `chosen_idx`: an index into the 2048 alpha vectors. `chosen_action`: an index into the 16 actions.
All inputs are finite; a program needn't handle non-finite values.
Results may differ from the reference program's by a relative error of at most 0.0003.
Values may be sent and summed in bfloat16 or wider, within the bound.
No kernel may reach another device: no remote copies, remote signals or barrier semaphores. Data moves between devices by JAX's collectives and lax.ppermute only.
A program may use at most 192 MiB of HBM per device.

```python
import math
import jax
import jax.numpy as jnp
from jax import lax

S = 2048
A = 16
O = 256
K = 2048
BEL = 1536


def touch_ends(result, stream_key, low, largest):
    spot = [jax.random.randint(jax.random.fold_in(stream_key, axis), (), 0, length) for axis, length in enumerate(result.shape)]
    widest = result.shape.index(max(result.shape))
    next_to = spot[:widest] + [(spot[widest] + 1) % result.shape[widest]] + spot[widest + 1:]
    return result.at[tuple(spot)].set(low).at[tuple(next_to)].set(largest)


def levels(stream_key, shape, pieces, smallest, top_value):
    def one(axis_at, blocks):
        draws = jax.random.uniform(jax.random.fold_in(jax.random.fold_in(stream_key, 6), axis_at), (blocks,), jnp.float32, smallest / len(pieces), top_value / len(pieces))
        return jnp.repeat(jnp.exp(draws), shape[axis_at] // blocks).reshape((-1,) + (1,) * (len(shape) - axis_at - 1))

    gain = one(*pieces[0])
    for cut in pieces[1:]:
        gain = gain * one(*cut)
    return gain


def bell_draw(key, dims, spread, most, split=(), kind=jnp.bfloat16):
    gain = levels(key, dims, split, -0.22, 0.18) if split else 1.0
    array = jax.random.normal(key, dims, jnp.float32) * spread * gain
    return jnp.minimum(jnp.maximum(array, -most), most).astype(kind)


def setup_inputs(seed: int = 0) -> dict:
    streams_of = jax.random.split(jax.random.key(seed), 7)
    alpha_set = bell_draw(streams_of[0], (K, S), 100.0, 600.0, ((0, 4),))
    transitions = jnp.clip(jnp.exp(math.log(1.0) - 6.9083047 * jax.random.uniform(streams_of[1], (A, S, S), jnp.float32) ** levels(streams_of[1], (A, S, S), ((1, 8),), -0.2, 0.2)), 0.0009994507, 1.0).astype(jnp.bfloat16)
    obs_weights = jnp.clip(jnp.exp(math.log(1.0) - 4.6051702 * jax.random.uniform(streams_of[2], (O, A, S), jnp.float32) ** levels(streams_of[2], (O, A, S), ((0, 8),), -0.2, 0.2)), 0.01, 1.0)
    rewards = jnp.clip(jax.random.uniform(streams_of[3], (A, S), jnp.float32, -1.0, 1.0), -1.0, 1.0)
    chosen_idx = touch_ends(jax.random.randint(streams_of[4], (BEL, A, O), 0, K), jax.random.fold_in(streams_of[4], 1), 0, K - 1).astype(jnp.int32)
    chosen_action = touch_ends(jax.random.randint(streams_of[5], (BEL,), 0, A), jax.random.fold_in(streams_of[5], 1), 0, A - 1).astype(jnp.int32)
    return {"alpha_set": alpha_set, "transitions": transitions, "obs_weights": obs_weights, "rewards": rewards, "chosen_idx": chosen_idx, "chosen_action": chosen_action}


discount = 0.95


def reference(alpha_set, transitions, obs_weights, rewards, chosen_idx, chosen_action):
    obs_prob = obs_weights / jnp.sum(obs_weights, axis=0, keepdims=True)
    trans_raw = transitions.astype(jnp.float32)
    trans_prob = trans_raw / jnp.sum(trans_raw, axis=1, keepdims=True)
    picked = jnp.take_along_axis(chosen_idx, chosen_action[:, None, None], axis=1)[:, 0, :]

    def add_obs(total, index):
        rows = jnp.take(alpha_set, picked[:, index], axis=0).astype(jnp.float32)
        probs = jnp.take(obs_prob[index], chosen_action, axis=0)
        return total + probs * rows, None

    start = jnp.zeros((BEL, S), jnp.float32)
    weighted, _ = lax.scan(add_obs, start, jnp.arange(O, dtype=jnp.int32))
    action_hot = (chosen_action[:, None] == jnp.arange(A, dtype=jnp.int32)[None, :]).astype(jnp.float32)

    def add_action(total, index):
        block = lax.dynamic_index_in_dim(trans_prob, index, 0, keepdims=False)
        moved = jnp.dot(weighted, block, precision=lax.Precision.HIGHEST, preferred_element_type=jnp.float32)
        column = lax.dynamic_slice_in_dim(action_hot, index, 1, 1)
        return total + column * moved, None

    future, _ = lax.scan(add_action, jnp.zeros((BEL, S), jnp.float32), jnp.arange(A, dtype=jnp.int32))
    reward_rows = jnp.take(rewards, chosen_action, axis=0)
    return reward_rows + discount * future
```

```python
import functools
import math

import jax
import jax.numpy as jnp
from jax import lax
from jax.experimental import pallas as pl
from jax.experimental.pallas import tpu as pltpu
from jax.sharding import PartitionSpec as P

discount = 0.95
LANES = 128
WEIGHT_LOW = 0.01
SPAN = -math.log2(WEIGHT_LOW)
FULL = 32767.0
FINE = 8.0
DIRECT = 4


def log_code(values, top):
    place = (jnp.log2(values) - math.log2(top) + SPAN) * (65535.0 / SPAN)
    return (jnp.clip(jnp.round(place), 0.0, 65535.0) - 32768.0).astype(jnp.int32).astype(jnp.int16)


def log_value(code, top):
    place = code.astype(jnp.int32).astype(jnp.float32) + 32768.0
    return jnp.exp2(place * (SPAN / 65535.0) + (math.log2(top) - SPAN))


def step_code(values, axis):
    most = jnp.max(jnp.abs(values), axis=axis, keepdims=True)
    power = jnp.ceil(jnp.log2(jnp.maximum(most, 1e-30)) * FINE + 0.01)
    steps = jnp.round(values * (jnp.exp2(power * (-1.0 / FINE)) * FULL))
    steps = jnp.clip(steps, -FULL, FULL)
    return power, steps.astype(jnp.int32).astype(jnp.int16)


def step_value(code, power):
    scale = jnp.exp2(power.astype(jnp.int32).astype(jnp.float32) * (1.0 / FINE)) * (1.0 / FULL)
    return code.astype(jnp.int32).astype(jnp.float32) * scale


def to_short(power):
    return power.astype(jnp.int32).astype(jnp.int16)


def lane_code(values):
    power, code = step_code(values, -1)
    tail = jnp.broadcast_to(to_short(power), values.shape[:-1] + (LANES,))
    return jnp.concatenate([code, tail], axis=-1)


def lane_value(message, width):
    return step_value(message[..., :width], message[..., width : width + 1])


def columns_of(array, inner_at, inner, outer):
    width = array.shape[-1] // (inner * outer)
    cuts = [
        lax.dynamic_slice_in_dim(array, (place * inner + inner_at) * width, width, array.ndim - 1)
        for place in range(outer)
    ]
    return jnp.concatenate(cuts, axis=-1)


def selecting_kernel(depth, act_ref, idx_ref, kept_ref, got_ref, *refs):
    *pieces, out_ref, totals_ref, table, w_table, inverse = refs
    rows, half = out_ref.shape[0], out_ref.shape[1] * out_ref.shape[2]
    tile = out_ref.shape[1]
    actions = totals_ref.shape[0]
    kept_rows = kept_ref.shape[0]

    @pl.when(pl.program_id(0) == 0)
    def _():
        base = 0
        for piece in pieces:
            step = math.gcd(piece.shape[0], 32)

            def widen(at, carry, piece=piece, base=base, step=step):
                block = piece[pl.ds(at * step, step)].astype(jnp.float32)
                table[pl.ds((base + at * step) * tile, step * tile)] = block.reshape(step * tile, LANES)
                return carry

            lax.fori_loop(0, piece.shape[0] // step, widen, 0)
            base += piece.shape[0]

        def lay(at, block):
            block = block.reshape(actions, tile, LANES)
            for kind in range(actions):
                w_table[pl.ds((kind * depth + at) * tile, tile)] = block[kind]

        def keep(at, total):
            block = kept_ref[pl.ds(at * actions, actions)]
            lay(at, block)
            return total + block

        def take(at, total):
            block = log_value(got_ref[pl.ds(at * actions, actions)], 1.0)
            lay(at + kept_rows // actions, block)
            return total + block

        total = jnp.zeros((actions, half), jnp.float32)
        total = lax.fori_loop(0, kept_rows // actions, keep, total)
        total = lax.fori_loop(0, kept_rows // actions, take, total)
        totals_ref[...] = total
        inverse[...] = (1.0 / total).reshape(actions * tile, LANES)

    first = pl.program_id(0) * rows

    def one(row, carry):
        kind = act_ref[first + row]
        at = pl.multiple_of(kind * (depth * tile), depth * tile)
        listed = idx_ref.at[pl.ds((first + row) * depth, depth)]
        parts = []
        for o in range(depth):
            place = pl.multiple_of(listed[o], tile)
            term = w_table[pl.ds(at + o * tile, tile)] * table[pl.ds(place, tile)]
            if o < 4:
                parts.append(term)
            else:
                parts[o % 4] = parts[o % 4] + term
        total = parts[0]
        for part in parts[1:]:
            total = total + part
        out_ref[row] = total * inverse[pl.ds(pl.multiple_of(kind * tile, tile), tile)]
        return carry

    lax.fori_loop(0, rows, one, 0, unroll=4)


def select_and_sum(actions, picks, kept, got, pieces, count, kinds):
    half = kept.shape[1]
    depth = picks.shape[0] // count
    tiles = pieces[0].shape[1:]
    step = math.gcd(count, 32)
    known = sum(piece.shape[0] for piece in pieces)
    whole = [pl.BlockSpec(memory_space=pltpu.VMEM) for _ in range(2 + len(pieces))]
    return pl.pallas_call(
        functools.partial(selecting_kernel, depth),
        grid=(count // step,),
        in_specs=[
            pl.BlockSpec(memory_space=pltpu.SMEM),
            pl.BlockSpec(memory_space=pltpu.SMEM),
            *whole,
        ],
        out_specs=[
            pl.BlockSpec((step,) + tiles, lambda g: (g, 0, 0)),
            pl.BlockSpec((kinds, half), lambda g: (0, 0)),
        ],
        out_shape=[
            jax.ShapeDtypeStruct((count,) + tiles, jnp.float32),
            jax.ShapeDtypeStruct((kinds, half), jnp.float32),
        ],
        scratch_shapes=[
            pltpu.VMEM((known * tiles[0], LANES), jnp.float32),
            pltpu.VMEM((depth * kinds * tiles[0], LANES), jnp.float32),
            pltpu.VMEM((kinds * tiles[0], LANES), jnp.float32),
        ],
        compiler_params=pltpu.CompilerParams(
            dimension_semantics=("arbitrary",), vmem_limit_bytes=48 * 1024 * 1024
        ),
        name="select_and_sum",
    )(actions, picks, kept, got, *pieces)


def body(alpha_set, transitions, obs_weights, rewards, chosen_idx, chosen_action):
    actions, states = rewards.shape
    obs_local = obs_weights.shape[0]
    bel_rows = chosen_action.shape[0]
    known_local = alpha_set.shape[0]
    ranks = lax.axis_size("obs")
    groups = lax.axis_size("bel")
    inner = 2
    outer = ranks // inner
    me = lax.axis_index("obs")
    outer_at, inner_at = me // inner, lax.rem(me, inner)
    seat = lax.axis_index("bel")
    width = states // ranks
    half = states // inner
    tiles = (half // LANES, LANES)
    depth = obs_local * inner
    owned = bel_rows // ranks

    def swap_inner(array):
        return lax.ppermute(array, "obs", [(i, i ^ 1) for i in range(ranks)])

    def shift_outer(array, k):
        hops = [(i, ((i // inner + k) % outer) * inner + i % inner) for i in range(ranks)]
        return lax.ppermute(array, "obs", hops)

    def exchange_outer(blocks):
        if outer <= DIRECT:
            return [shift_outer(blocks(lax.rem(outer_at + k, outer)), k) for k in range(1, outer)]
        teams = [[q * inner + r for q in range(outer)] for r in range(inner)]
        sent = jnp.stack([blocks(jnp.int32(place)) for place in range(outer)])
        got = lax.all_to_all(sent, "obs", 0, 0, tiled=True, axis_index_groups=teams)
        got = lax.dynamic_slice_in_dim(jnp.concatenate([got, got]), outer_at, outer, 0)
        return [got[k] for k in range(1, outer)]

    mine = columns_of(alpha_set, inner_at, inner, outer).reshape((known_local,) + tiles)
    pieces, order, distance = [mine], [0], groups // 2
    while distance:
        hops = [(i, i ^ distance) for i in range(groups)]
        pieces = pieces + [lax.ppermute(piece, "bel", hops) for piece in pieces]
        order = order + [place ^ distance for place in order]
        distance //= 2

    action_hot = (chosen_action[:, None] == jnp.arange(actions, dtype=jnp.int32)[None, :])
    picks = jnp.sum(jnp.where(action_hot[:, :, None], chosen_idx, 0), axis=1)
    action_hot = action_hot.astype(jnp.float32)

    kept = columns_of(obs_weights, inner_at, inner, outer).reshape(obs_local * actions, half)
    given = log_code(columns_of(obs_weights, 1 - inner_at, inner, outer), 1.0)
    given = given.reshape(obs_local * actions, half)
    listed = picks.astype(jnp.int16).reshape(-1)
    pad = -listed.shape[0] % (16 * half)
    listed_rows = jnp.pad(listed, (0, pad)).reshape(-1, half)
    got = swap_inner(jnp.concatenate([given, listed_rows], axis=0))
    got_picks = got[obs_local * actions :].reshape(-1)[: listed.shape[0]].astype(jnp.int32).reshape(bel_rows, obs_local)

    share = jnp.sum(transitions.astype(jnp.float32), axis=1)
    if outer <= DIRECT:
        trans_totals = share
        for k in range(1, outer):
            trans_totals = trans_totals + shift_outer(share, k)
        trans_totals = trans_totals + swap_inner(trans_totals)
    else:
        trans_totals = lax.psum(share, "obs")

    both_picks = jnp.concatenate([picks, got_picks], axis=1)
    block, inside = both_picks // known_local, lax.rem(both_picks, known_local)
    relative = block ^ seat
    place = jnp.zeros_like(relative)
    for at, member in enumerate(order):
        place = jnp.where(relative == member, at, place)
    rows = (place * known_local + inside) * tiles[0]
    rows, trans_totals = lax.optimization_barrier((rows, trans_totals))
    shares, here_totals = select_and_sum(
        chosen_action, rows.reshape(-1), kept, got, pieces, bel_rows, actions
    )
    shares = shares.reshape(bel_rows, half)

    power, code = step_code(shares, 0)
    message = jnp.concatenate(
        [code, log_code(here_totals, float(depth)), jnp.broadcast_to(to_short(power), (16, half))], axis=0
    )
    received = exchange_outer(lambda q: lax.dynamic_slice_in_dim(message, q * width, width, 1))
    parts = [lax.dynamic_slice_in_dim(shares, outer_at * width, width, 1)]
    totals = [lax.dynamic_slice_in_dim(here_totals, outer_at * width, width, 1)]
    for block in received:
        parts.append(step_value(block[:bel_rows], block[bel_rows + actions : bel_rows + actions + 1]))
        totals.append(log_value(block[bel_rows : bel_rows + actions], float(depth)))
    factors = jnp.dot(action_hot, jnp.concatenate(totals, axis=1), precision=lax.Precision.HIGHEST)
    above, below = 0.0, 0.0
    for at, part in enumerate(parts):
        factor = factors[:, at * width : (at + 1) * width]
        above, below = above + factor * part, below + factor
    weighted = above / below

    upper = lax.reduce_precision(weighted, 8, 7)
    lower = weighted - upper
    halves = jnp.stack([upper, lower]).astype(jnp.bfloat16)
    spread = (action_hot.astype(jnp.bfloat16)[None, :, :, None] * halves[:, :, None, :]).reshape(
        2 * bel_rows, actions * width
    )
    moved = jnp.dot(
        spread, transitions.reshape(actions * width, states), preferred_element_type=jnp.float32
    )
    inverse = jnp.dot(action_hot, 1.0 / trans_totals, precision=lax.Precision.HIGHEST)
    future = (moved[:bel_rows] + moved[bel_rows:]) * inverse

    future = future.reshape(outer, inner, owned, states)
    ours = lax.dynamic_index_in_dim(future, inner_at, 1, keepdims=False)
    theirs = lane_code(lax.dynamic_index_in_dim(future, 1 - inner_at, 1, keepdims=False))
    ours = ours + lane_value(swap_inner(theirs), states)
    coded = lane_code(ours)
    total = lax.dynamic_index_in_dim(ours, outer_at, 0, keepdims=False)
    for block in exchange_outer(lambda q: lax.dynamic_index_in_dim(coded, q, 0, keepdims=False)):
        total = total + lane_value(block, states)
    own_hot = lax.dynamic_slice_in_dim(action_hot, me * owned, owned, 0)
    reward_rows = jnp.dot(own_hot, rewards, precision=lax.Precision.HIGHEST)
    return reward_rows + discount * total


def solution(mesh):
    placed = (
        P("bel", None),
        P(None, "obs", None),
        P("obs", None, None),
        P(),
        P("bel", None, "obs"),
        P("bel"),
    )
    return jax.shard_map(
        body, mesh=mesh, in_specs=placed, out_specs=P(("bel", "obs"), None), check_vma=False
    )
```

```python
import math

import jax
import jax.numpy as jnp
from jax import lax
from jax.experimental import pallas as pl
from jax.experimental.pallas import tpu as pltpu
from jax.sharding import PartitionSpec as P


discount = 0.95
LANES = 128
WEIGHT_LOW = 0.01
SPAN = -math.log2(WEIGHT_LOW)
FULL = 32767.0
FINE = 8.0
DIRECT = 4


def log_code(values, top):
    place = (jnp.log2(values) - math.log2(top) + SPAN) * (65535.0 / SPAN)
    return (jnp.clip(jnp.round(place), 0.0, 65535.0) - 32768.0).astype(jnp.int32).astype(jnp.int16)


def log_value(code, top):
    place = code.astype(jnp.int32).astype(jnp.float32) + 32768.0
    return jnp.exp2(place * (SPAN / 65535.0) + (math.log2(top) - SPAN))


def step_code(values, axis):
    most = jnp.max(jnp.abs(values), axis=axis, keepdims=True)
    power = jnp.ceil(jnp.log2(jnp.maximum(most, 1e-30)) * FINE + 0.01)
    steps = jnp.round(values * (jnp.exp2(power * (-1.0 / FINE)) * FULL))
    steps = jnp.clip(steps, -FULL, FULL)
    return power, steps.astype(jnp.int32).astype(jnp.int16)


def step_value(code, power):
    scale = jnp.exp2(power.astype(jnp.int32).astype(jnp.float32) * (1.0 / FINE)) * (1.0 / FULL)
    return code.astype(jnp.int32).astype(jnp.float32) * scale


def to_short(power):
    return power.astype(jnp.int32).astype(jnp.int16)


def lane_code(values):
    power, code = step_code(values, -1)
    tail = jnp.broadcast_to(to_short(power), values.shape[:-1] + (LANES,))
    return jnp.concatenate([code, tail], axis=-1)


def lane_value(message, width):
    return step_value(message[..., :width], message[..., width : width + 1])


def columns_of(array, inner_at, inner, outer):
    width = array.shape[-1] // (inner * outer)
    cuts = [
        lax.dynamic_slice_in_dim(array, (place * inner + inner_at) * width, width, array.ndim - 1)
        for place in range(outer)
    ]
    return jnp.concatenate(cuts, axis=-1)


def selecting_kernel(act_ref, own_idx_ref, got_idx_ref, kept_ref, got_ref, *refs):
    *pieces, out_ref, totals_ref, table, w_table, inverse = refs
    rows, half = out_ref.shape[0], out_ref.shape[1] * out_ref.shape[2]
    tile = out_ref.shape[1]
    actions = totals_ref.shape[0]
    kept_rows = kept_ref.shape[0]
    near = kept_rows // actions
    depth = 2 * near

    @pl.when(pl.program_id(0) == 0)
    def _():
        base = 0
        for piece in pieces:
            step = math.gcd(piece.shape[0], 32)

            def widen(at, carry, piece=piece, base=base, step=step):
                block = piece[pl.ds(at * step, step)].astype(jnp.float32)
                table[pl.ds((base + at * step) * tile, step * tile)] = block.reshape(step * tile, LANES)
                return carry

            lax.fori_loop(0, piece.shape[0] // step, widen, 0)
            base += piece.shape[0]

        def lay(at, block):
            block = block.reshape(actions, tile, LANES)
            for kind in range(actions):
                w_table[pl.ds((kind * depth + at) * tile, tile)] = block[kind]

        def keep(at, total):
            block = kept_ref[pl.ds(at * actions, actions)]
            lay(at, block)
            return total + block

        def take(at, total):
            block = log_value(got_ref[pl.ds(at * actions, actions)], 1.0)
            lay(at + kept_rows // actions, block)
            return total + block

        total = jnp.zeros((actions, half), jnp.float32)
        total = lax.fori_loop(0, kept_rows // actions, keep, total)
        total = lax.fori_loop(0, kept_rows // actions, take, total)
        totals_ref[...] = total
        inverse[...] = (1.0 / total).reshape(actions * tile, LANES)

    first = pl.program_id(0) * rows
    span = own_idx_ref.shape[0] - near + 1
    spots = [ref.at[pl.ds(o, span)] for ref in (own_idx_ref, got_idx_ref) for o in range(near)]

    def one(row, carry):
        kind = act_ref[first + row]
        at = pl.multiple_of(kind * (depth * tile), depth * tile)
        listed = (first + row) * near
        parts = []
        for o in range(depth):
            place = pl.multiple_of(spots[o][listed], tile)
            term = w_table[pl.ds(at + o * tile, tile)] * table[pl.ds(place, tile)]
            if o < 4:
                parts.append(term)
            else:
                parts[o % 4] = parts[o % 4] + term
        total = parts[0]
        for part in parts[1:]:
            total = total + part
        out_ref[row] = total * inverse[pl.ds(pl.multiple_of(kind * tile, tile), tile)]
        return carry

    lax.fori_loop(0, rows, one, 0, unroll=4)


def select_and_sum(actions, own_picks, got_picks, kept, got, pieces, kinds):
    half = kept.shape[1]
    count = actions.shape[0]
    depth = 2 * kept.shape[0] // kinds
    tiles = pieces[0].shape[1:]
    step = math.gcd(count, 32)
    known = sum(piece.shape[0] for piece in pieces)
    whole = [pl.BlockSpec(memory_space=pltpu.VMEM) for _ in range(2 + len(pieces))]
    return pl.pallas_call(
        selecting_kernel,
        grid=(count // step,),
        in_specs=[
            pl.BlockSpec(memory_space=pltpu.SMEM),
            pl.BlockSpec(memory_space=pltpu.SMEM),
            pl.BlockSpec(memory_space=pltpu.SMEM),
            *whole,
        ],
        out_specs=[
            pl.BlockSpec((step,) + tiles, lambda g: (g, 0, 0)),
            pl.BlockSpec((kinds, half), lambda g: (0, 0)),
        ],
        out_shape=[
            jax.ShapeDtypeStruct((count,) + tiles, jnp.float32),
            jax.ShapeDtypeStruct((kinds, half), jnp.float32),
        ],
        scratch_shapes=[
            pltpu.VMEM((known * tiles[0], LANES), jnp.float32),
            pltpu.VMEM((depth * kinds * tiles[0], LANES), jnp.float32),
            pltpu.VMEM((kinds * tiles[0], LANES), jnp.float32),
        ],
        compiler_params=pltpu.CompilerParams(
            dimension_semantics=("arbitrary",), vmem_limit_bytes=48 * 1024 * 1024
        ),
        name="select_and_sum",
    )(actions, own_picks, got_picks, kept, got, *pieces)


def moving_kernel(kinds_ref, halves_ref, trans_ref, inverse_ref, out_ref, spread):
    rows = out_ref.shape[0]
    actions, width, columns = trans_ref.shape

    @pl.when(pl.program_id(0) == 0)
    def _():
        for kind in range(actions):
            held = jnp.where(kinds_ref[...] == kind, halves_ref[...], 0.0)
            spread[:, kind * width : (kind + 1) * width] = held.astype(jnp.bfloat16)

    product = jnp.dot(
        spread[...], trans_ref[...].reshape(actions * width, columns), preferred_element_type=jnp.float32
    )
    kinds = lax.broadcasted_iota(jnp.int32, (rows, actions), 1)
    hot = (kinds_ref[:rows] == kinds).astype(jnp.float32)
    factor = jnp.dot(
        hot, inverse_ref[...], precision=lax.Precision.HIGHEST, preferred_element_type=jnp.float32
    )
    out_ref[...] = (product[:rows] + product[rows:]) * factor


def move(kinds, weighted, transitions, inverse):
    rows, width = weighted.shape
    actions, _, states = transitions.shape
    upper = lax.reduce_precision(weighted, 8, 7)
    halves = jnp.concatenate([upper, weighted - upper])
    columns = math.gcd(states, 512)
    return pl.pallas_call(
        moving_kernel,
        grid=(states // columns,),
        in_specs=[
            pl.BlockSpec(memory_space=pltpu.VMEM),
            pl.BlockSpec(memory_space=pltpu.VMEM),
            pl.BlockSpec((actions, width, columns), lambda n: (0, 0, n)),
            pl.BlockSpec((actions, columns), lambda n: (0, n)),
        ],
        out_specs=pl.BlockSpec((rows, columns), lambda n: (0, n)),
        out_shape=jax.ShapeDtypeStruct((rows, states), jnp.float32),
        scratch_shapes=[pltpu.VMEM((2 * rows, actions * width), jnp.bfloat16)],
        compiler_params=pltpu.CompilerParams(
            dimension_semantics=("arbitrary",), vmem_limit_bytes=48 * 1024 * 1024
        ),
        name="move",
    )(jnp.concatenate([kinds, kinds])[:, None], halves, transitions, inverse)


def backup(alpha_set, transitions, obs_weights, rewards, chosen_idx, chosen_action):
    actions, states = rewards.shape
    obs_local = obs_weights.shape[0]
    bel_rows = chosen_action.shape[0]
    known_local = alpha_set.shape[0]
    ranks = lax.axis_size("obs")
    groups = lax.axis_size("bel")
    inner = 2
    outer = ranks // inner
    me = lax.axis_index("obs")
    outer_at, inner_at = me // inner, lax.rem(me, inner)
    seat = lax.axis_index("bel")
    width = states // ranks
    half = states // inner
    tiles = (half // LANES, LANES)
    depth = obs_local * inner
    owned = bel_rows // ranks

    def swap_inner(array):
        return lax.ppermute(array, "obs", [(i, i ^ 1) for i in range(ranks)])

    def shift_outer(array, k):
        hops = [(i, ((i // inner + k) % outer) * inner + i % inner) for i in range(ranks)]
        return lax.ppermute(array, "obs", hops)

    def exchange_outer(blocks):
        if outer <= DIRECT:
            return [shift_outer(blocks(lax.rem(outer_at + k, outer)), k) for k in range(1, outer)]
        teams = [[q * inner + r for q in range(outer)] for r in range(inner)]
        sent = jnp.stack([blocks(jnp.int32(place)) for place in range(outer)])
        got = lax.all_to_all(sent, "obs", 0, 0, tiled=True, axis_index_groups=teams)
        got = lax.dynamic_slice_in_dim(jnp.concatenate([got, got]), outer_at, outer, 0)
        return [got[k] for k in range(1, outer)]

    mine = columns_of(alpha_set, inner_at, inner, outer).reshape((known_local,) + tiles)
    pieces, order, distance = [mine], [0], groups // 2
    while distance:
        hops = [(i, i ^ distance) for i in range(groups)]
        pieces = pieces + [lax.ppermute(piece, "bel", hops) for piece in pieces]
        order = order + [place ^ distance for place in order]
        distance //= 2

    action_hot = (chosen_action[:, None] == jnp.arange(actions, dtype=jnp.int32)[None, :])
    picks = jnp.sum(jnp.where(action_hot[:, :, None], chosen_idx, 0), axis=1)
    action_hot = action_hot.astype(jnp.float32)
    relative = (picks // known_local) ^ seat
    place = jnp.zeros_like(relative)
    for at, member in enumerate(order):
        place = jnp.where(relative == member, at, place)
    own_rows = ((place * known_local + lax.rem(picks, known_local)) * tiles[0]).reshape(-1)
    got_rows = swap_inner(own_rows)

    kept = columns_of(obs_weights, inner_at, inner, outer).reshape(obs_local * actions, half)
    given = log_code(columns_of(obs_weights, 1 - inner_at, inner, outer), 1.0)
    given, late = lax.optimization_barrier((given.reshape(obs_local * actions, half), transitions))
    got = swap_inner(given)

    share = jnp.sum(late.astype(jnp.float32), axis=1)
    if outer <= DIRECT:
        column_share = share
        for k in range(1, outer):
            column_share = column_share + shift_outer(share, k)
        own_rows, column_share = lax.optimization_barrier((own_rows, column_share))
        trans_totals = column_share + swap_inner(column_share)
    else:
        trans_totals = lax.psum(share, "obs")

    shares, here_totals = select_and_sum(chosen_action, own_rows, got_rows, kept, got, pieces, actions)
    shares = shares.reshape(bel_rows, half)

    power, code = step_code(shares, 0)
    message = jnp.concatenate(
        [code, log_code(here_totals, float(depth)), jnp.broadcast_to(to_short(power), (16, half))], axis=0
    )
    received = exchange_outer(lambda q: lax.dynamic_slice_in_dim(message, q * width, width, 1))
    parts = [lax.dynamic_slice_in_dim(shares, outer_at * width, width, 1)]
    totals = [lax.dynamic_slice_in_dim(here_totals, outer_at * width, width, 1)]
    for block in received:
        parts.append(step_value(block[:bel_rows], block[bel_rows + actions : bel_rows + actions + 1]))
        totals.append(log_value(block[bel_rows : bel_rows + actions], float(depth)))
    factors = jnp.dot(action_hot, jnp.concatenate(totals, axis=1), precision=lax.Precision.HIGHEST)
    above, below = 0.0, 0.0
    for at, part in enumerate(parts):
        factor = factors[:, at * width : (at + 1) * width]
        above, below = above + factor * part, below + factor
    weighted = above / below

    def rows_of(array, at):
        array = array.reshape((outer, inner, owned) + array.shape[1:])
        array = lax.dynamic_index_in_dim(array, at, 1, keepdims=False)
        array = lax.dynamic_slice_in_dim(jnp.concatenate([array, array]), outer_at, outer, 0)
        return array.reshape((outer * owned,) + array.shape[2:])

    inverse = 1.0 / trans_totals
    theirs = lane_code(
        move(rows_of(chosen_action, 1 - inner_at), rows_of(weighted, 1 - inner_at), transitions, inverse)
    )
    ours = move(rows_of(chosen_action, inner_at), rows_of(weighted, inner_at), transitions, inverse)
    cut = outer // 2
    far = swap_inner(theirs[cut * owned :])
    near = swap_inner(theirs[: cut * owned])
    far = lane_code(ours[cut * owned :] + lane_value(far, states))
    if outer <= DIRECT:
        blocks = [shift_outer(far[k * owned : (k + 1) * owned], cut + k) for k in range(outer - cut)]
        total = ours[:owned] + lane_value(near[:owned], states)
        near = lane_code(ours[owned : cut * owned] + lane_value(near[owned:], states))
        blocks += [shift_outer(near[k * owned : (k + 1) * owned], 1 + k) for k in range(cut - 1)]
    else:
        near = ours[: cut * owned] + lane_value(near, states)
        total = near[:owned]
        coded = jnp.concatenate([lane_code(near), far]).reshape(outer, owned, -1)
        blocks = exchange_outer(
            lambda q: lax.dynamic_index_in_dim(coded, lax.rem(q - outer_at + outer, outer), 0, keepdims=False)
        )
    for block in blocks:
        total = total + lane_value(block, states)
    own_hot = lax.dynamic_slice_in_dim(action_hot, me * owned, owned, 0)
    reward_rows = jnp.dot(own_hot, rewards, precision=lax.Precision.HIGHEST)
    return reward_rows + discount * total


def solution(mesh):
    placed = (
        P("bel", None),
        P(None, "obs", None),
        P("obs", None, None),
        P(),
        P("bel", None, "obs"),
        P("bel"),
    )
    return jax.shard_map(backup, mesh=mesh, in_specs=placed, out_specs=P(("bel", "obs"), None), check_vma=False)
```
